32 devices in a mesh: tp: 8 (over y, x, core), dp: 4 (over z).
Axes of the slice: x: 2, y: 2, z: 4, core: 2. Of those that a mesh axis runs over, the one named last changes fastest.
Arguments:
- grad_out: bfloat16 [512, 16384], P('dp', 'tp'), may hold values from -6 to 6
- hidden_sum: bfloat16 [512, 16384], P('dp', 'tp'), may hold values from -100 to 100
- norm_gain: float32 [16384], P('tp'), may hold values from 0.5 to 1.5
- out_weight: bfloat16 [2048, 16384], P(None, 'tp'), may hold values from -0.046875 to 0.046875
Outputs:
- resid_grad: bfloat16 [512, 16384], P('dp', 'tp')
- attn_grad: bfloat16 [512, 2048], P('dp', 'tp')
- gain_grad: float32 [16384], P('tp')
The draws below stay inside these ranges and needn't reach their ends.
All inputs are finite; a program needn't handle non-finite values.
Results may differ from the reference program's by a relative error of at most 0.0049.
Values sent between devices are 32-bit elements; how exact they have to be, the bound alone decides.
No kernel may reach another device: no remote copies, remote signals or barrier semaphores. Data moves between devices by JAX's collectives and lax.ppermute only.
A program may use at most 64 MiB of HBM per device.

```python
import math
import jax
import jax.numpy as jnp
from jax import lax

D = 16384
TOKENS = 512
D_IN = 2048


def draw_hidden_sum(key, part):
    key_values, key_row, key_col = jax.random.split(jax.random.fold_in(key, 11), 3)
    position = jnp.arange(D, dtype=jnp.float32) / D
    column = jnp.exp(math.log(3.0) * position + math.log(10.0) * jax.random.uniform(key_col, (D,), jnp.float32))
    column = column / jnp.sqrt(jnp.mean(column * column))
    values = jnp.clip(jax.random.normal(key_values, (TOKENS, D), jnp.float32), -4.0, 4.0)
    row_scale = jnp.exp(jax.random.uniform(key_row, (TOKENS, 1), jnp.float32, minval=math.log(0.3), maxval=math.log(3.0)))
    return jnp.clip(values * row_scale * column, -100.0, 100.0).astype(jnp.bfloat16)


def steps_of(own_key, dims, cuts, low, largest):
    level = 1.0
    for dim, blocks in cuts:
        steps = jax.random.uniform(jax.random.fold_in(jax.random.fold_in(own_key, 6), dim), (blocks,), jnp.float32, low / len(cuts), largest / len(cuts))
        level = level * jnp.repeat(jnp.exp(steps), dims[dim] // blocks).reshape((-1,) + (1,) * (len(dims) - 1 - dim))
    return level


def normal_values(own_key, dims, deviation, most, cuts=(), kind=jnp.bfloat16):
    array = deviation * jax.random.normal(own_key, dims, jnp.float32)
    if cuts:
        array = array * steps_of(own_key, dims, cuts, -0.22, 0.18)
    return jnp.clip(array, -most, most).astype(kind)


def setup_inputs(seed: int = 0) -> dict:
    seeds = jax.random.split(jax.random.key(seed), 5)
    grad_out = normal_values(seeds[0], (TOKENS, D), 1.0, 6.0, ((0, 4), (1, 8)))
    hidden_sum = draw_hidden_sum(jax.random.fold_in(seeds[4], 71), 0)
    norm_gain = jnp.clip(0.5 + 1.0 * jax.random.uniform(seeds[2], (D,), jnp.float32) ** steps_of(seeds[2], (D,), ((0, 8),), -0.2, 0.2), 0.5, 1.5)
    out_weight = normal_values(seeds[3], (D_IN, D), D ** -0.5, 0.046875, ((1, 8),))
    return dict(grad_out=grad_out, hidden_sum=hidden_sum, norm_gain=norm_gain, out_weight=out_weight)


epsilon = 1e-05

def backward_rows(upstream_b, stream_b, norm_gain, out_weight):
    upstream = upstream_b.astype(jnp.float32)
    stream = stream_b.astype(jnp.float32)
    squares = lax.optimization_barrier(jnp.sum(stream * stream, axis=1))
    inverse = lax.rsqrt(squares / D + epsilon)
    dotted = lax.optimization_barrier(jnp.sum(norm_gain * upstream * stream, axis=1))
    factor = inverse * inverse * dotted / D
    resid_full = inverse[:, None] * (norm_gain * upstream - stream * factor[:, None])
    resid_grad = resid_full.astype(jnp.bfloat16)
    attn_grad = jnp.dot(resid_grad, out_weight.T, preferred_element_type=jnp.float32).astype(jnp.bfloat16)
    gain_part = lax.optimization_barrier(jnp.sum(upstream * stream * inverse[:, None], axis=0))
    return (resid_grad, attn_grad, gain_part)

def reference(grad_out, hidden_sum, norm_gain, out_weight):
    span_rows = math.gcd(TOKENS, 512)
    number = TOKENS // span_rows

    def advance(carry, pieces):
        resid_grad, attn_grad, gain_part = backward_rows(pieces[0], pieces[1], norm_gain, out_weight)
        return (carry + gain_part, (resid_grad, attn_grad))
    gain_grad, outputs = lax.scan(advance, jnp.zeros((D,), jnp.float32), (grad_out.reshape(number, span_rows, D), hidden_sum.reshape(number, span_rows, D)))
    return (outputs[0].reshape(TOKENS, D), outputs[1].reshape(TOKENS, D_IN), gain_grad)
```

```python
import jax
import jax.numpy as jnp
from jax import lax
from jax.experimental import pallas as pl
from jax.experimental.pallas import tpu as pltpu
from jax.sharding import PartitionSpec as P

epsilon = 1e-05
ROWS = 16


def products_kernel(go_hbm, hs_hbm, gain_hbm, w_hbm, st_ref, out_ref, go, hs, gain, w, x, cols, in_sems, w_sems):
    tokens, width = go.shape
    blocks, n, _ = w.shape
    loads = [
        pltpu.make_async_copy(src, dst, in_sems.at[i])
        for i, (src, dst) in enumerate(((go_hbm, go), (hs_hbm, hs), (gain_hbm, gain)))
    ]
    streams = [
        pltpu.make_async_copy(w_hbm.at[pl.ds(j * n, n), :], w.at[j], w_sems.at[j]) for j in range(blocks)
    ]
    for copy in loads + streams:
        copy.start()
    for copy in loads:
        copy.wait()
    for t in range(0, tokens, ROWS):
        rows = pl.ds(t, ROWS)
        stream_b = hs[rows, :]
        stream = stream_b.astype(jnp.float32)
        scaled = gain[...] * go[rows, :].astype(jnp.float32)
        square = jnp.sum(stream * stream, axis=1, keepdims=True)
        dotted = jnp.sum(scaled * stream, axis=1, keepdims=True)
        factor = dotted / (square + epsilon * width)
        x[rows, :] = (scaled - stream * factor).astype(jnp.bfloat16)
        x[pl.ds(tokens + t, ROWS), :] = stream_b
        cols[0, rows, :] = square
        cols[1, rows, :] = dotted
        cols[2, rows, :] = factor
    diagonal = lax.broadcasted_iota(jnp.int32, (tokens, tokens), 0) == lax.broadcasted_iota(
        jnp.int32, (tokens, tokens), 1
    )
    for i in range(2):
        st_ref[i : i + 1, :] = jnp.sum(jnp.where(diagonal, cols[i], 0.0), axis=0, keepdims=True)
    for j in range(blocks):
        streams[j].wait()
        both = lax.dot_general(x[...], w[j], (((1,), (1,)), ((), ())), preferred_element_type=jnp.float32)
        second = both[tokens:]
        out_ref[j % 2, 0, j // 2] = both[:tokens] + cols[2] * second
        out_ref[j % 2, 1, j // 2] = second


def products(go, hs, gain, w, blocks):
    tokens, width = go.shape
    n = w.shape[0] // blocks
    return pl.pallas_call(
        products_kernel,
        out_shape=(
            jax.ShapeDtypeStruct((2, tokens), jnp.float32),
            jax.ShapeDtypeStruct((2, 2, blocks // 2, tokens, n), jnp.float32),
        ),
        in_specs=[pl.BlockSpec(memory_space=pl.ANY)] * 4,
        out_specs=(pl.BlockSpec(memory_space=pltpu.VMEM), pl.BlockSpec(memory_space=pltpu.VMEM)),
        scratch_shapes=[
            pltpu.VMEM((tokens, width), jnp.bfloat16),
            pltpu.VMEM((tokens, width), jnp.bfloat16),
            pltpu.VMEM((1, width), jnp.float32),
            pltpu.VMEM((blocks, n, width), jnp.bfloat16),
            pltpu.VMEM((2 * tokens, width), jnp.bfloat16),
            pltpu.VMEM((3, tokens, 1), jnp.float32),
            pltpu.SemaphoreType.DMA((3,)),
            pltpu.SemaphoreType.DMA((blocks,)),
        ],
    )(go, hs, gain.reshape(1, width), w)


def swap(value, axis, size, mask):
    return lax.ppermute(value, axis, [(i, i ^ mask(i)) for i in range(size)])


def build(tp, dp):
    bits = tp.bit_length() - 1

    def on_device(grad_out, hidden_sum, norm_gain, out_weight):
        features = grad_out.shape[1] * tp
        me = lax.axis_index("tp")
        stats, pair = products(grad_out, hidden_sum, norm_gain, out_weight, tp)

        low = me & 1
        stats = stats + swap(stats, "tp", tp, lambda i: 1)
        from_pair = swap(lax.dynamic_index_in_dim(pair, 1 - low, 0, False), "tp", tp, lambda i: 1)
        for bit in range(1, bits):
            stats = stats + swap(stats, "tp", tp, lambda i: 1 << bit)
        inverse = lax.rsqrt(stats[0] / features + epsilon)
        factor = inverse * inverse * stats[1] / features

        pair = lax.dynamic_index_in_dim(pair, low, 0, False) + from_pair
        partial = inverse[:, None] * (pair[0] - factor[:, None] * pair[1])

        upper = me >> 1
        count = bits - 1
        def order(i, step):
            return step if i & 1 == 0 else count - 1 - step

        current = None
        for step in range(count):
            free = count - step - 1

            def pick(own, step=step, free=free, source=current):
                mine = jnp.where(low == 0, upper >> order(0, step), upper >> order(1, step)) & 1
                wanted = mine if own else 1 - mine
                if source is None:
                    pieces = []
                    for offset in range(1 << free):
                        def spell(parity):
                            number = wanted << order(parity, step)
                            for k, s in enumerate(range(step + 1, count)):
                                number = number | (((offset >> k) & 1) << order(parity, s))
                            return number
                        number = jnp.where(low == 0, spell(0), spell(1))
                        pieces.append(lax.dynamic_index_in_dim(partial, number, 0, True))
                    return jnp.concatenate(pieces, 0) if len(pieces) > 1 else pieces[0]
                shaped = source.reshape((1 << free, 2) + source.shape[1:])
                return lax.dynamic_index_in_dim(shaped, wanted, 1, False)

            got = swap(pick(False), "tp", tp, lambda i: 2 << order(i, step))
            current = pick(True) + got
        attn_grad = current[0].astype(jnp.bfloat16)

        upstream = grad_out.astype(jnp.float32)
        stream = hidden_sum.astype(jnp.float32)
        resid_grad = (
            inverse[:, None] * (norm_gain * upstream - stream * factor[:, None])
        ).astype(jnp.bfloat16)
        gain_grad = jnp.sum(upstream * stream * inverse[:, None], axis=0)
        mask = 1
        while mask < dp:
            gain_grad = gain_grad + swap(gain_grad, "dp", dp, lambda i: mask)
            mask *= 2
        return (resid_grad, attn_grad, gain_grad)

    return on_device


def solution(mesh):
    return jax.shard_map(
        build(mesh.shape["tp"], mesh.shape["dp"]),
        mesh=mesh,
        in_specs=(P("dp", "tp"), P("dp", "tp"), P("tp"), P(None, "tp")),
        out_specs=(P("dp", "tp"), P("dp", "tp"), P("tp")),
        check_vma=False,
    )
```

```python
import jax
import jax.numpy as jnp
from jax import lax
from jax.experimental import pallas as pl
from jax.experimental.pallas import tpu as pltpu
from jax.sharding import PartitionSpec as P

epsilon = 1e-05
VMEM = 64 << 20
ROWS = 16
GROUP = 2
AHEAD = 4


def stats_kernel(go_hbm, hs_hbm, gain_hbm, st_ref, x, go, hs, gain, cols, sems):
    tokens, width = go.shape
    loads = [
        pltpu.make_async_copy(src, dst, sems.at[i])
        for i, (src, dst) in enumerate(((go_hbm, go), (hs_hbm, hs), (gain_hbm, gain)))
    ]
    for copy in loads:
        copy.start()
    for copy in loads:
        copy.wait()
    for t in range(0, tokens, ROWS):
        rows = pl.ds(t, ROWS)
        stream_b = hs[rows, :]
        stream = stream_b.astype(jnp.float32)
        scaled = gain[...] * go[rows, :].astype(jnp.float32)
        square = jnp.sum(stream * stream, axis=1, keepdims=True)
        dotted = jnp.sum(scaled * stream, axis=1, keepdims=True)
        factor = dotted / (square + epsilon * width)
        x[rows, :] = (scaled - stream * factor).astype(jnp.bfloat16)
        x[pl.ds(tokens + t, ROWS), :] = stream_b
        cols[0, rows, :] = square
        cols[1, rows, :] = dotted
        cols[2, rows, :] = factor
    diagonal = lax.broadcasted_iota(jnp.int32, (tokens, tokens), 0) == lax.broadcasted_iota(
        jnp.int32, (tokens, tokens), 1
    )
    for i in range(3):
        st_ref[i : i + 1, :] = jnp.sum(jnp.where(diagonal, cols[i], 0.0), axis=0, keepdims=True)


def local_stats(go, hs, gain):
    tokens, width = go.shape
    return pl.pallas_call(
        stats_kernel,
        out_shape=(pltpu.VMEM((3, tokens), jnp.float32), pltpu.VMEM((2 * tokens, width), jnp.bfloat16)),
        in_specs=[pl.BlockSpec(memory_space=pltpu.HBM)] * 3,
        out_specs=(pl.BlockSpec(memory_space=pltpu.VMEM),) * 2,
        scratch_shapes=[
            pltpu.VMEM((tokens, width), jnp.bfloat16),
            pltpu.VMEM((tokens, width), jnp.bfloat16),
            pltpu.VMEM((1, width), jnp.float32),
            pltpu.VMEM((3, tokens, 1), jnp.float32),
            pltpu.SemaphoreType.DMA((3,)),
        ],
        compiler_params=pltpu.CompilerParams(vmem_limit_bytes=VMEM - 4 * tokens * width - (3 << 17)),
        cost_estimate=pl.CostEstimate(flops=8 * tokens * width, bytes_accessed=4 * tokens * width, transcendentals=0),
    )(go, hs, gain.reshape(1, width))


def products_kernel(low_ref, st_ref, x, w_hbm, give_ref, keep_ref, w, sems):
    tokens = st_ref.shape[1]
    blocks, n, width = w.shape
    group = min(GROUP, blocks)
    low, half = low_ref[0], blocks // 2

    def load(j):
        source = 2 * (j % half) + (1 - low if j < half else low)
        return pltpu.make_async_copy(w_hbm.at[pl.ds(source * n, n), :], w.at[j], sems.at[j])

    loads = [load(j) for j in range(blocks)]
    for copy in loads[:AHEAD]:
        copy.start()
    for g in range(0, blocks, group):
        for j in range(g, g + group):
            loads[j].wait()
            if j + AHEAD < blocks:
                loads[j + AHEAD].start()
        both = lax.dot_general(
            w[g : g + group].reshape(group * n, width),
            x[...],
            (((1,), (1,)), ((), ())),
            preferred_element_type=jnp.float32,
        )
        for k in range(group):
            j = g + k
            part = both[k * n : (k + 1) * n]
            second = part[:, tokens:]
            out = give_ref if j < half else keep_ref
            out[0, j % half] = part[:, :tokens] + st_ref[2:3, :] * second
            out[1, j % half] = second


def products(low, stats, x, w, blocks):
    tokens = stats.shape[1]
    rows, width = w.shape
    n = rows // blocks
    vmem = pl.BlockSpec(memory_space=pltpu.VMEM)
    return pl.pallas_call(
        products_kernel,
        out_shape=(pltpu.VMEM((2, blocks // 2, n, tokens), jnp.float32),) * 2,
        in_specs=[pl.BlockSpec(memory_space=pltpu.SMEM), vmem, vmem, pl.BlockSpec(memory_space=pltpu.HBM)],
        out_specs=(vmem, vmem),
        scratch_shapes=[pltpu.VMEM((blocks, n, width), jnp.bfloat16), pltpu.SemaphoreType.DMA((blocks,))],
        compiler_params=pltpu.CompilerParams(vmem_limit_bytes=VMEM - 16 * tokens * rows // 2 - 4 * tokens * width - (3 << 20)),
        cost_estimate=pl.CostEstimate(
            flops=4 * tokens * rows * width, bytes_accessed=2 * rows * width, transcendentals=0
        ),
    )(low.reshape(1), stats, pltpu.with_memory_space_constraint(x, pltpu.VMEM), w)


def swap(value, axis, size, mask):
    return lax.ppermute(value, axis, [(i, i ^ mask(i)) for i in range(size)])


def build(tp, dp):
    count = tp.bit_length() - 2

    def order(i, step):
        return step if i & 1 == 0 else count - 1 - step

    def body(grad_out, hidden_sum, norm_gain, out_weight):
        features = grad_out.shape[1] * tp
        me = lax.axis_index("tp")
        low, upper = me & 1, me >> 1
        local, x = local_stats(grad_out, hidden_sum, norm_gain)
        stats = local[:2] + swap(local[:2], "tp", tp, lambda i: 1)
        local, x, stats = lax.optimization_barrier((local, x, stats))
        give, keep = products(low, local, x, out_weight, tp)
        for bit in range(1, count + 1):
            other = swap(stats, "tp", tp, lambda i: 1 << bit)
            stats = stats + other
        from_pair = swap(give, "tp", tp, lambda i: 1)
        inverse = lax.rsqrt(stats[0] / features + epsilon)
        factor = inverse * inverse * stats[1] / features

        pair = keep + from_pair
        partial = inverse * (pair[0] - factor * pair[1])

        def wanted(step, own):
            mine = jnp.where(low == 0, upper >> order(0, step), upper >> order(1, step)) & 1
            return mine if own else 1 - mine

        def blocks_of(step, bit):
            pieces = []
            for offset in range(1 << (count - step - 1)):
                def number(parity):
                    value = bit << order(parity, step)
                    for k, s in enumerate(range(step + 1, count)):
                        value = value | (((offset >> k) & 1) << order(parity, s))
                    return value

                which = jnp.where(low == 0, number(0), number(1))
                pieces.append(lax.dynamic_index_in_dim(partial, which, 0, True))
            return jnp.concatenate(pieces, 0) if len(pieces) > 1 else pieces[0]

        def halve(source, step, own):
            if step == 0:
                return blocks_of(step, wanted(step, own))
            shaped = source.reshape((-1, 2) + source.shape[1:])
            return lax.dynamic_index_in_dim(shaped, wanted(step, own), 1, False)

        current, sums = None, None
        for step in range(count):
            given = halve(current, step, False)
            if step == 1:
                given, sums = lax.optimization_barrier((given, sums))
            got = swap(given, "tp", tp, lambda i: 2 << order(i, step))
            if step == 0:
                upstream = grad_out.astype(jnp.float32)
                stream = hidden_sum.astype(jnp.float32)
                resid_grad = (
                    inverse[:, None] * (norm_gain * upstream - stream * factor[:, None])
                ).astype(jnp.bfloat16)
                sums = jnp.sum(upstream * stream * inverse[:, None], axis=0)
                if dp > 1:
                    sums = sums + swap(sums, "dp", dp, lambda i: 1)
            current = halve(current, step, True) + got
        attn_grad = current[0].T.astype(jnp.bfloat16)
        mask = 2
        while mask < dp:
            sums = sums + swap(sums, "dp", dp, lambda i: mask)
            mask *= 2
        return (resid_grad, attn_grad, sums)

    return body


def solution(mesh):
    return jax.shard_map(
        build(mesh.shape["tp"], mesh.shape["dp"]),
        mesh=mesh,
        in_specs=(P("dp", "tp"), P("dp", "tp"), P("tp"), P(None, "tp")),
        out_specs=(P("dp", "tp"), P("dp", "tp"), P("tp")),
        check_vma=False,
    )
```

```python
import functools

import jax
import jax.numpy as jnp
from jax import lax
from jax.experimental import pallas as pl
from jax.experimental.pallas import tpu as pltpu
from jax.sharding import PartitionSpec as P

epsilon = 1e-05
VMEM = 64 << 20
ROWS = 16
GROUP = 2


def stats_kernel(go_hbm, hs_hbm, gain_hbm, st_ref, x, go, hs, gain, cols, sems):
    tokens, width = go.shape
    loads = [
        pltpu.make_async_copy(src, dst, sems.at[i])
        for i, (src, dst) in enumerate(((go_hbm, go), (hs_hbm, hs), (gain_hbm, gain)))
    ]
    for copy in loads:
        copy.start()
    for copy in loads:
        copy.wait()
    for t in range(0, tokens, ROWS):
        rows = pl.ds(t, ROWS)
        stream_b = hs[rows, :]
        stream = stream_b.astype(jnp.float32)
        scaled = gain[...] * go[rows, :].astype(jnp.float32)
        square = jnp.sum(stream * stream, axis=1, keepdims=True)
        dotted = jnp.sum(scaled * stream, axis=1, keepdims=True)
        factor = dotted / (square + epsilon * width)
        x[rows, :] = (scaled - stream * factor).astype(jnp.bfloat16)
        x[pl.ds(tokens + t, ROWS), :] = stream_b
        cols[0, rows, :] = square
        cols[1, rows, :] = dotted
        cols[2, rows, :] = factor
    diagonal = lax.broadcasted_iota(jnp.int32, (tokens, tokens), 0) == lax.broadcasted_iota(
        jnp.int32, (tokens, tokens), 1
    )
    for i in range(3):
        st_ref[i : i + 1, :] = jnp.sum(jnp.where(diagonal, cols[i], 0.0), axis=0, keepdims=True)


def local_stats(go, hs, gain):
    tokens, width = go.shape
    return pl.pallas_call(
        stats_kernel,
        out_shape=(pltpu.VMEM((3, tokens), jnp.float32), pltpu.VMEM((2 * tokens, width), jnp.bfloat16)),
        in_specs=[pl.BlockSpec(memory_space=pltpu.HBM)] * 3,
        out_specs=(pl.BlockSpec(memory_space=pltpu.VMEM),) * 2,
        scratch_shapes=[
            pltpu.VMEM((tokens, width), jnp.bfloat16),
            pltpu.VMEM((tokens, width), jnp.bfloat16),
            pltpu.VMEM((1, width), jnp.float32),
            pltpu.VMEM((3, tokens, 1), jnp.float32),
            pltpu.SemaphoreType.DMA((3,)),
        ],
        compiler_params=pltpu.CompilerParams(vmem_limit_bytes=VMEM - 4 * tokens * width - (3 << 17)),
        cost_estimate=pl.CostEstimate(flops=8 * tokens * width, bytes_accessed=4 * tokens * width, transcendentals=0),
    )(go, hs, gain.reshape(1, width))


def products_kernel(flip, st_ref, x, w_hbm, out_ref, w, sems):
    tokens = st_ref.shape[1]
    half, n, width = w.shape
    group = min(GROUP, half)
    parity = (lax.axis_index("tp") + flip) % 2

    def load(j):
        return pltpu.make_async_copy(w_hbm.at[pl.ds((2 * j + parity) * n, n), :], w.at[j], sems.at[j])

    loads = [load(j) for j in range(half)]
    for copy in loads:
        copy.start()
    for g in range(0, half, group):
        for j in range(g, g + group):
            loads[j].wait()
        both = lax.dot_general(
            w[g : g + group].reshape(group * n, width),
            x[...],
            (((1,), (1,)), ((), ())),
            preferred_element_type=jnp.float32,
        )
        for k in range(group):
            part = both[k * n : (k + 1) * n]
            second = part[:, tokens:]
            out_ref[0, g + k] = part[:, :tokens] + st_ref[2:3, :] * second
            out_ref[1, g + k] = second


def products(flip, stats, x, w, blocks):
    tokens = stats.shape[1]
    rows, width = w.shape
    n, half = rows // blocks, blocks // 2
    vmem = pl.BlockSpec(memory_space=pltpu.VMEM)
    return pl.pallas_call(
        functools.partial(products_kernel, flip),
        out_shape=pltpu.VMEM((2, half, n, tokens), jnp.float32),
        in_specs=[vmem, vmem, pl.BlockSpec(memory_space=pltpu.HBM)],
        out_specs=vmem,
        scratch_shapes=[pltpu.VMEM((half, n, width), jnp.bfloat16), pltpu.SemaphoreType.DMA((half,))],
        compiler_params=pltpu.CompilerParams(
            vmem_limit_bytes=VMEM - 16 * tokens * rows // 2 - 4 * tokens * width - (3 << 20)
        ),
        cost_estimate=pl.CostEstimate(
            flops=2 * tokens * rows * width, bytes_accessed=rows * width, transcendentals=0
        ),
    )(
        pltpu.with_memory_space_constraint(stats, pltpu.VMEM), pltpu.with_memory_space_constraint(x, pltpu.VMEM), w
    )


def swap(value, axis, size, mask):
    return lax.ppermute(value, axis, [(i, i ^ mask(i)) for i in range(size)])


def build(tp, dp):
    count = tp.bit_length() - 2

    def order(i, step):
        return step if i & 1 == 0 else count - 1 - step

    def body(grad_out, hidden_sum, norm_gain, out_weight):
        features = grad_out.shape[1] * tp
        me = lax.axis_index("tp")
        low, upper = me & 1, me >> 1
        local, x = local_stats(grad_out, hidden_sum, norm_gain)
        stats = local[:2] + swap(local[:2], "tp", tp, lambda i: 1)
        local, x, stats = lax.optimization_barrier((local, x, stats))
        give = products(1, local, x, out_weight, tp)
        keep = products(0, local, x, out_weight, tp)
        for bit in range(1, count + 1):
            other = swap(stats, "tp", tp, lambda i: 1 << bit)
            stats = stats + other
        from_pair = swap(give, "tp", tp, lambda i: 1)
        inverse = lax.rsqrt(stats[0] / features + epsilon)
        factor = inverse * inverse * stats[1] / features

        pair = keep + from_pair
        partial = inverse * (pair[0] - factor * pair[1])

        def wanted(step, own):
            mine = jnp.where(low == 0, upper >> order(0, step), upper >> order(1, step)) & 1
            return mine if own else 1 - mine

        def blocks_of(step, bit):
            pieces = []
            for offset in range(1 << (count - step - 1)):
                def number(parity):
                    value = bit << order(parity, step)
                    for k, s in enumerate(range(step + 1, count)):
                        value = value | (((offset >> k) & 1) << order(parity, s))
                    return value

                which = jnp.where(low == 0, number(0), number(1))
                pieces.append(lax.dynamic_index_in_dim(partial, which, 0, True))
            return jnp.concatenate(pieces, 0) if len(pieces) > 1 else pieces[0]

        def halve(source, step, own):
            if step == 0:
                return blocks_of(step, wanted(step, own))
            shaped = source.reshape((-1, 2) + source.shape[1:])
            return lax.dynamic_index_in_dim(shaped, wanted(step, own), 1, False)

        current, sums = None, None
        for step in range(count):
            given = halve(current, step, False)
            if step == 1:
                given, sums = lax.optimization_barrier((given, sums))
            got = swap(given, "tp", tp, lambda i: 2 << order(i, step))
            if step == 0:
                upstream = grad_out.astype(jnp.float32)
                stream = hidden_sum.astype(jnp.float32)
                resid_grad = (
                    inverse[:, None] * (norm_gain * upstream - stream * factor[:, None])
                ).astype(jnp.bfloat16)
                sums = jnp.sum(upstream * stream * inverse[:, None], axis=0)
                if dp > 1:
                    sums = sums + swap(sums, "dp", dp, lambda i: 1)
            current = halve(current, step, True) + got
        attn_grad = current[0].T.astype(jnp.bfloat16)
        mask = 2
        while mask < dp:
            sums = sums + swap(sums, "dp", dp, lambda i: mask)
            mask *= 2
        return (resid_grad, attn_grad, sums)

    return body


def solution(mesh):
    return jax.shard_map(
        build(mesh.shape["tp"], mesh.shape["dp"]),
        mesh=mesh,
        in_specs=(P("dp", "tp"), P("dp", "tp"), P("tp"), P(None, "tp")),
        out_specs=(P("dp", "tp"), P("dp", "tp"), P("tp")),
        check_vma=False,
    )
```
